128 devices in a mesh: py: 4 (over y), pz: 32 (over z, x, core).
Axes of the slice: x: 4, y: 4, z: 4, core: 2. Of those that a mesh axis runs over, the one named last changes fastest.
Arguments:
- species: float32 [4, 512, 256, 256], P(None, None, 'py', 'pz'), may hold values from -6 to 6
- coupling: float32 [4, 4], replicated, may hold values from -4 to 4
- symbol_x: float32 [512], replicated, may hold values from 0.3 to 3
- symbol_y: float32 [256], replicated, may hold values from 0.3 to 3
- symbol_z: float32 [256], replicated, may hold values from 0.3 to 3
Outputs:
- modes: float32 [4, 512, 256, 256], P(None, 'py', 'pz')
The draws below stay inside these ranges and needn't reach their ends.
All inputs are finite; a program needn't handle non-finite values.
Results may differ from the reference program's by a relative error of at most 0.00007.
Values sent between devices are 32-bit elements; how exact they have to be, the bound alone decides.
A program may use at most 64 MiB of HBM per device.

```python
import jax
import jax.numpy as jnp
from jax import lax

GRID_X = 512
GRID_Y = 256
GRID_Z = 256
FIELDS = 4


def block_levels(key, shape, pieces, low, largest):
    def one(dim, shards_of):
        draws = jax.random.uniform(jax.random.fold_in(jax.random.fold_in(key, 6), dim), (shards_of,), jnp.float32, low / len(pieces), largest / len(pieces))
        return jnp.repeat(jnp.exp(draws), shape[dim] // shards_of).reshape((-1,) + (1,) * (len(shape) - dim - 1))

    gain = one(*pieces[0])
    for cut in pieces[1:]:
        gain = gain * one(*cut)
    return gain


def bell_draw(rng, shape, spread, most, shards=(), dtype=jnp.bfloat16):
    result = spread * jax.random.normal(rng, shape, jnp.float32)
    if shards:
        result = result * block_levels(rng, shape, shards, -0.22, 0.18)
    return jnp.clip(result, -most, most).astype(dtype)


def setup_inputs(seed: int = 0) -> dict:
    key_list = jax.random.split(jax.random.key(seed), 6)
    return {
        "species": bell_draw(key_list[0], (FIELDS, GRID_X, GRID_Y, GRID_Z), 1.0, 6.0, ((2, 4), (3, 32)), jnp.float32),
        "coupling": bell_draw(key_list[1], (FIELDS, FIELDS), 0.7, 4.0, (), jnp.float32),
        "symbol_x": jnp.clip(jax.random.uniform(key_list[2], (GRID_X,), jnp.float32, 0.3, 3.0), 0.3, 3.0),
        "symbol_y": jnp.clip(jax.random.uniform(key_list[3], (GRID_Y,), jnp.float32, 0.3, 3.0), 0.3, 3.0),
        "symbol_z": jnp.clip(jax.random.uniform(key_list[4], (GRID_Z,), jnp.float32, 0.3, 3.0), 0.3, 3.0),
    }


def mode_table(count):
    rank = jnp.arange(count)
    angle = (jnp.pi / (4 * count)) * (((2 * rank[:, None] + 1) * (2 * rank[None, :] + 1)) % (8 * count)).astype(jnp.float32)
    return jnp.cos(angle) * (2.0 / count) ** 0.5


def transform_dim(values, dim):
    moved = jnp.tensordot(values, mode_table(values.shape[dim]), axes=([dim], [0]), precision=lax.Precision.HIGHEST)
    return jnp.moveaxis(moved, -1, dim)


def reference(species, coupling, symbol_x, symbol_y, symbol_z):
    modes = species
    modes = transform_dim(modes, 1)
    modes = transform_dim(modes, 2)
    modes = transform_dim(modes, 3)
    symbol = symbol_x[:, None, None] + symbol_y[None, :, None] + symbol_z[None, None, :]
    weight_xyz = 1.0 / (1.0 + symbol)
    mixed_fields = jnp.einsum("ab,bxyz->axyz", coupling, modes, precision=lax.Precision.HIGHEST)
    modes = weight_xyz * modes + (1.0 - weight_xyz) * mixed_fields
    return modes
```

```python
import functools

import jax
import jax.numpy as jnp
import numpy as np
from jax import lax
from jax.experimental import pallas as pl
from jax.experimental.pallas import tpu as pltpu
from jax.sharding import PartitionSpec as P

MESH = pl.DeviceIdType.MESH
F32 = jnp.float32
BF16 = jnp.bfloat16


def mode_table(count):
    rank = 2 * np.arange(count, dtype=np.int64) + 1
    angle = (rank[:, None] * rank[None, :] % (8 * count)) * (np.pi / (4 * count))
    return (np.cos(angle) * np.sqrt(2.0 / count)).astype(np.float32)


def halves(table):
    high = table.astype(BF16)
    low = (table - high.astype(np.float32)).astype(BF16)
    return np.concatenate([high, low], axis=0)


def split(values):
    high = values.astype(BF16)
    low = (values - high.astype(F32)).astype(BF16)
    return high, low


def dot(lhs, rhs):
    return jnp.dot(lhs, rhs, preferred_element_type=F32)


def exchange_kernel(
    species_ref, hx_hbm, hy_hbm, hz_hbm, modes_ref,
    xin, hx, hy, hz, lhs_high, lhs_low, ysend, yrecv, p1send, p1recv, final,
    in_sem, table_sem, ys_sem, yr_sem, p1s_sem, p1r_sem, p2s_sem, p2r_sem,
):
    me_y = lax.axis_index("py")
    me_pz = lax.axis_index("pz")
    me_z = me_pz // 8
    me_x = (me_pz // 2) % 4
    me_c = me_pz % 2

    def at(z, x, c):
        return (me_y, z * 8 + x * 2 + c)

    def load_field(field):
        return [
            pltpu.make_async_copy(
                species_ref.at[field, :, :, pl.ds(128 * tile, 128)],
                xin.at[field, tile],
                in_sem.at[field, tile],
            )
            for tile in range(4)
        ]

    tables = [
        pltpu.make_async_copy(hx_hbm, hx, table_sem.at[0]),
        pltpu.make_async_copy(hy_hbm, hy, table_sem.at[1]),
        pltpu.make_async_copy(hz_hbm, hz, table_sem.at[2]),
    ]
    for copy in load_field(0):
        copy.start()
    tables[0].start()

    barrier = pltpu.get_barrier_semaphore()
    peers = [(lax.rem(me_y + d, 4), me_pz) for d in (1, 2, 3)]
    for d in (1, 2, 3):
        for c in (0, 1):
            peers.append(at(me_z, lax.rem(me_x + d, 4), c))
            peers.append(at(lax.rem(me_z + d, 4), me_x, c))
    peers.append(at(me_z, me_x, 1 - me_c))
    for peer in peers:
        pl.semaphore_signal(barrier, inc=1, device_id=peer, device_id_type=MESH)

    for field in (1, 2, 3):
        for copy in load_field(field):
            copy.start()
    tables[1].start()
    tables[2].start()
    tables[0].wait()

    def x_stage(field):
        for copy in load_field(field):
            copy.wait()
        for z in range(8):
            for tile in range(4):
                rows = xin.at[field, tile].reshape(512, 128)[pl.ds(z, 64, stride=8), :]
                high, low = split(rows)
                lhs_high[pl.ds(64 * z, 64), pl.ds(128 * tile, 128)] = high
                lhs_low[pl.ds(64 * z, 64), pl.ds(128 * tile, 128)] = low
        for half in range(2):
            high = lhs_high[pl.ds(256 * half, 256), :]
            low = lhs_low[pl.ds(256 * half, 256), :]
            for side in range(2):
                columns = pl.ds(256 * side, 256)
                table = hx[pl.ds(0, 512), columns]
                out = dot(high, table) + dot(low, table)
                out += dot(high, hx[pl.ds(512, 512), columns])
                for plane in range(4):
                    for part in range(2):
                        ysend[
                            field * 4 + half * 2 + plane // 2, side * 2 + part, plane % 2
                        ] = out[64 * plane : 64 * plane + 64, 128 * part : 128 * part + 128]

    def y_send(piece):
        for d in (1, 3, 2):
            to = lax.rem(me_y + d, 4)
            pltpu.make_async_remote_copy(
                src_ref=ysend.at[piece, to],
                dst_ref=yrecv.at[piece, :, me_y],
                send_sem=ys_sem.at[piece],
                recv_sem=yr_sem.at[piece],
                device_id=(to, me_pz),
                device_id_type=MESH,
            ).start()
        yrecv[piece, :, me_y] = ysend[piece, me_y]

    x_stage(0)
    pl.semaphore_wait(barrier, len(peers))
    for piece in range(4):
        y_send(piece)

    @pl.loop(1, 4)
    def _(field):
        x_stage(field)
        for pair in range(4):
            y_send(field * 4 + pair)

    tables[1].wait()
    tables[2].wait()

    def y_stage(piece):
        all_y = yrecv.at[piece, :, pl.ds(0, 3)]
        pltpu.make_async_copy(all_y, all_y, yr_sem.at[piece]).wait()
        data = jnp.concatenate(
            [yrecv[piece, plane].reshape(256, 128) for plane in range(2)], axis=1
        )
        high, low = split(data)
        out = dot(hy[pl.ds(0, 256), :], high) + dot(hy[pl.ds(256, 256), :], high)
        out += dot(hy[pl.ds(0, 256), :], low)
        for plane in range(2):
            p1send[piece, :, :, :, plane] = out[:, 128 * plane : 128 * plane + 128].reshape(
                4, 4, 2, 8, 128
            )

    def first_send(piece, along_x):
        for d in (1, 3, 2):
            if along_x:
                to = lax.rem(me_x + d, 4)
                src, device = p1send.at[piece, :, to], at(me_z, to, me_c)
                dst = p1recv.at[piece, me_x]
            else:
                to = lax.rem(me_z + d, 4)
                src, device = p1send.at[piece, to], at(to, me_x, me_c)
                dst = p1recv.at[piece, me_z]
            pltpu.make_async_remote_copy(
                src_ref=src, dst_ref=dst,
                send_sem=p1s_sem.at[piece], recv_sem=p1r_sem.at[piece],
                device_id=device, device_id_type=MESH,
            ).start()
        if along_x:
            p1recv[piece, me_x] = p1send[piece, :, me_x]
        else:
            p1recv[piece, me_z] = p1send[piece, me_z]

    def second_send(piece, along_x):
        arrived = p1recv.at[piece, pl.ds(0, 3)]
        pltpu.make_async_copy(arrived, arrived, p1r_sem.at[piece]).wait()
        for d in (1, 3, 2, 0):
            for c in (me_c, 1 - me_c):
                if along_x:
                    to = lax.rem(me_x + d, 4)
                    device, dst = at(me_z, to, c), final.at[piece, :, me_x, me_c]
                else:
                    to = lax.rem(me_z + d, 4)
                    device, dst = at(to, me_x, c), final.at[piece, me_z, :, me_c]
                if d == 0 and c is me_c:
                    continue
                pltpu.make_async_remote_copy(
                    src_ref=p1recv.at[piece, :, to, c], dst_ref=dst,
                    send_sem=p2s_sem.at[piece], recv_sem=p2r_sem.at[piece],
                    device_id=device, device_id_type=MESH,
                ).start()
        if along_x:
            final[piece, :, me_x, me_c] = p1recv[piece, :, me_x, me_c]
        else:
            final[piece, me_z, :, me_c] = p1recv[piece, :, me_z, me_c]

    def z_stage(field):
        for pair in range(4):
            arrived = final.at[field * 4 + pair].reshape(512, 128).at[pl.ds(0, 448)]
            pltpu.make_async_copy(arrived, arrived, p2r_sem.at[field * 4 + pair]).wait()
        for ky in range(8):
            data = jnp.concatenate(
                [
                    final.at[field * 4 + pair].reshape(512, 128)[pl.ds(ky, 64, stride=8), :]
                    for pair in range(4)
                ],
                axis=0,
            )
            high, low = split(data.T)
            table = hz[pl.ds(0, 256), :]
            out = dot(high, table) + dot(low, table) + dot(high, hz[pl.ds(256, 256), :])
            for part in range(2):
                modes_ref.at[field, part].reshape(1024, 128)[pl.ds(ky, 128, stride=8), :] = out[
                    :, 128 * part : 128 * part + 128
                ]

    def second_pair(step):
        second_send(2 * step, False)
        second_send(2 * step + 1, True)

    @pl.loop(0, 4)
    def _(field):
        for half in range(2):
            step = 2 * field + half
            if half == 0:
                @pl.when(field > 0)
                def _():
                    second_pair(step - 1)
            else:
                second_pair(step - 1)
            y_stage(2 * step)
            first_send(2 * step, True)
            y_stage(2 * step + 1)
            first_send(2 * step + 1, False)
            if half == 0:
                @pl.when(field >= 2)
                def _():
                    z_stage(field - 2)

    second_pair(7)
    z_stage(2)
    z_stage(3)

    @pl.loop(0, 16)
    def _(piece):
        sent = ysend.at[piece, pl.ds(0, 3)]
        pltpu.make_async_copy(sent, sent, ys_sem.at[piece]).wait()
        sent = p1recv.at[piece, pl.ds(0, 3)]
        pltpu.make_async_copy(sent, sent, p1s_sem.at[piece]).wait()
        sent = final.at[piece].reshape(512, 128).at[pl.ds(0, 448)]
        pltpu.make_async_copy(sent, sent, p2s_sem.at[piece]).wait()


def exchange(species, hx, hy, hz):
    dma = pltpu.SemaphoreType.DMA
    anywhere = pl.BlockSpec(memory_space=pl.ANY)
    return pl.pallas_call(
        exchange_kernel,
        out_shape=jax.ShapeDtypeStruct((4, 2, 128, 8, 128), F32),
        in_specs=[anywhere] * 4,
        out_specs=pl.BlockSpec(memory_space=pltpu.VMEM),
        scratch_shapes=[
            pltpu.VMEM((4, 4, 64, 8, 128), F32),
            pltpu.VMEM((1024, 512), BF16),
            pltpu.VMEM((512, 256), BF16),
            pltpu.VMEM((512, 256), BF16),
            pltpu.VMEM((512, 512), BF16),
            pltpu.VMEM((512, 512), BF16),
            pltpu.VMEM((16, 4, 2, 64, 128), F32),
            pltpu.VMEM((16, 2, 4, 64, 128), F32),
            pltpu.VMEM((16, 4, 4, 2, 2, 8, 128), F32),
            pltpu.VMEM((16, 4, 4, 2, 2, 8, 128), F32),
            pltpu.VMEM((16, 4, 4, 2, 2, 8, 128), F32),
            dma((4, 4)),
            dma((3,)),
            dma((16,)),
            dma((16,)),
            dma((16,)),
            dma((16,)),
            dma((16,)),
            dma((16,)),
        ],
        compiler_params=pltpu.CompilerParams(
            collective_id=0, has_side_effects=True, vmem_limit_bytes=40 * 2**20
        ),
        name="exchange",
    )(species, hx, hy, hz)


def mix_kernel(modes_ref, coupling_ref, symbol_x_ref, symbol_yz_ref, out_ref):
    block = out_ref.shape[1]
    first = pl.program_id(0) * block

    @pl.loop(0, block)
    def _(row):
        for part in range(2):
            lanes = pl.ds(128 * part, 128)
            weight = 1.0 / (symbol_x_ref[first + row] + symbol_yz_ref[:, lanes])
            old = [modes_ref[a, part, row] for a in range(4)]
            for a in range(4):
                mixed = coupling_ref[a, 0] * old[0]
                for b in range(1, 4):
                    mixed += coupling_ref[a, b] * old[b]
                out_ref[a, row, :, lanes] = mixed + weight * (old[a] - mixed)


def mix(modes, coupling, part_x, symbol_yz):
    steps = 8
    block = 128 // steps
    smem = pl.BlockSpec(memory_space=pltpu.SMEM)
    return pl.pallas_call(
        mix_kernel,
        grid=(steps,),
        out_shape=jax.ShapeDtypeStruct((4, 128, 8, 256), F32),
        in_specs=[
            pl.BlockSpec((4, 2, block, 8, 128), lambda i: (0, 0, i, 0, 0)),
            smem,
            smem,
            pl.BlockSpec((8, 256), lambda i: (0, 0)),
        ],
        out_specs=pl.BlockSpec((4, block, 8, 256), lambda i: (0, i, 0, 0)),
        name="mix",
    )(modes, coupling, part_x, symbol_yz)


def shards(species, coupling, symbol_x, symbol_y, symbol_z):
    hx = halves(mode_table(512))
    hy = halves(mode_table(256))
    table_z = mode_table(256).reshape(32, 4, 2, 256).transpose(1, 0, 2, 3).reshape(256, 256)
    hz = halves(table_z)
    modes = exchange(species.transpose(0, 2, 3, 1), hx, hy, hz)
    part_x = lax.dynamic_slice_in_dim(symbol_x, lax.axis_index("py") * 128, 128)
    part_y = lax.dynamic_slice_in_dim(symbol_y, lax.axis_index("pz") * 8, 8)
    symbol_yz = 1.0 + part_y[:, None] + symbol_z[None, :]
    return mix(modes, coupling, part_x, symbol_yz)


def solution(mesh):
    return jax.shard_map(
        shards,
        mesh=mesh,
        in_specs=(P(None, None, "py", "pz"), P(), P(), P(), P()),
        out_specs=P(None, "py", "pz", None),
        check_vma=False,
    )
```

```python
import functools

import jax
import jax.numpy as jnp
import numpy as np
from jax import lax
from jax.experimental import pallas as pl
from jax.experimental.pallas import tpu as pltpu
from jax.sharding import PartitionSpec as P

MESH = pl.DeviceIdType.MESH
F32 = jnp.float32
BF16 = jnp.bfloat16
AHEAD = 3
LAG = 2


def mode_table(count):
    rank = 2 * np.arange(count, dtype=np.int64) + 1
    angle = (rank[:, None] * rank[None, :] % (8 * count)) * (np.pi / (4 * count))
    return (np.cos(angle) * np.sqrt(2.0 / count)).astype(np.float32)


def halves(table):
    high = table.astype(BF16)
    low = (table - high.astype(np.float32)).astype(BF16)
    return np.concatenate([high, low], axis=0)


def split(values):
    high = values.astype(BF16)
    low = (values - high.astype(F32)).astype(BF16)
    return high, low


def dot(lhs, rhs):
    return jnp.dot(lhs, rhs, preferred_element_type=F32)


def exchange_kernel(
    species_ref, table, modes_ref,
    xin, lhs_high, lhs_low, ysend, yrecv, p1send, p1recv, final,
    in_sem, ys_sem, yr_sem, p1s_sem, p1r_sem, p2s_sem, p2r_sem,
):
    me_y = lax.axis_index("py")
    me_pz = lax.axis_index("pz")
    me_z = me_pz // 8
    me_x = (me_pz // 2) % 4
    me_c = me_pz % 2

    def at(z, x, c):
        return (me_y, z * 8 + x * 2 + c)

    def load_field(field):
        return [
            pltpu.make_async_copy(
                species_ref.at[field, :, :, pl.ds(128 * tile, 128)],
                xin.at[field, tile],
                in_sem.at[field, tile],
            )
            for tile in range(4)
        ]

    y_high = table.at[pl.ds(1024, 256), pl.ds(0, 256)]
    y_low = table.at[pl.ds(1280, 256), pl.ds(0, 256)]
    z_high = table.at[pl.ds(1024, 256), pl.ds(256, 256)]
    z_low = table.at[pl.ds(1280, 256), pl.ds(256, 256)]

    for copy in load_field(0):
        copy.start()

    barrier = pltpu.get_barrier_semaphore()
    peers = [(lax.rem(me_y + d, 4), me_pz) for d in (1, 2, 3)]
    for d in (1, 2, 3):
        for c in (0, 1):
            peers.append(at(me_z, lax.rem(me_x + d, 4), c))
            peers.append(at(lax.rem(me_z + d, 4), me_x, c))
    peers.append(at(me_z, me_x, 1 - me_c))
    for peer in peers:
        pl.semaphore_signal(barrier, inc=1, device_id=peer, device_id_type=MESH)

    for field in (1, 2, 3):
        for copy in load_field(field):
            copy.start()

    def x_stage(field, half):
        for plane in range(4):
            for tile in range(4):
                rows = xin.at[field, tile].reshape(512, 128)[
                    pl.ds(4 * half + plane, 64, stride=8), :
                ]
                high, low = split(rows)
                lhs_high[pl.ds(64 * plane, 64), pl.ds(128 * tile, 128)] = high
                lhs_low[pl.ds(64 * plane, 64), pl.ds(128 * tile, 128)] = low
        for side in range(2):
            columns = pl.ds(256 * side, 256)
            x_high = table[pl.ds(0, 512), columns]
            out = dot(lhs_high[...], x_high) + dot(lhs_low[...], x_high)
            out += dot(lhs_high[...], table[pl.ds(512, 512), columns])
            for plane in range(4):
                for part in range(2):
                    ysend[
                        field * 4 + half * 2 + plane // 2, side * 2 + part, plane % 2
                    ] = out[64 * plane : 64 * plane + 64, 128 * part : 128 * part + 128]

    def y_send(piece):
        for d in (1, 3, 2):
            to = lax.rem(me_y + d, 4)
            pltpu.make_async_remote_copy(
                src_ref=ysend.at[piece, to],
                dst_ref=yrecv.at[piece, :, me_y],
                send_sem=ys_sem.at[piece],
                recv_sem=yr_sem.at[piece],
                device_id=(to, me_pz),
                device_id_type=MESH,
            ).start()
        yrecv[piece, :, me_y] = ysend[piece, me_y]

    def y_stage(piece):
        all_y = yrecv.at[piece, :, pl.ds(0, 3)]
        pltpu.make_async_copy(all_y, all_y, yr_sem.at[piece]).wait()
        data = jnp.concatenate(
            [yrecv[piece, plane].reshape(256, 128) for plane in range(2)], axis=1
        )
        high, low = split(data)
        out = dot(y_high[...], high) + dot(y_low[...], high) + dot(y_high[...], low)
        for plane in range(2):
            p1send[piece, plane] = out[:, 128 * plane : 128 * plane + 128].reshape(
                4, 4, 2, 8, 128
            )

    def first_send(piece):
        for d in (1, 3, 2):
            for plane in range(2):
                if plane == 0:
                    to = lax.rem(me_x + d, 4)
                    src, device = p1send.at[piece, 0, :, to], at(me_z, to, me_c)
                    dst = p1recv.at[piece, 0, me_x]
                else:
                    to = lax.rem(me_z + d, 4)
                    src, device = p1send.at[piece, 1, to], at(to, me_x, me_c)
                    dst = p1recv.at[piece, 1, me_z]
                pltpu.make_async_remote_copy(
                    src_ref=src, dst_ref=dst,
                    send_sem=p1s_sem.at[piece], recv_sem=p1r_sem.at[piece, plane],
                    device_id=device, device_id_type=MESH,
                ).start()
        p1recv[piece, 0, me_x] = p1send[piece, 0, :, me_x]
        p1recv[piece, 1, me_z] = p1send[piece, 1, me_z]

    def second_send(piece):
        for plane in range(2):
            arrived = p1recv.at[piece, plane, pl.ds(0, 3)]
            pltpu.make_async_copy(arrived, arrived, p1r_sem.at[piece, plane]).wait()
            for d in (1, 3, 2, 0):
                for c in (me_c, 1 - me_c):
                    if d == 0 and c is me_c:
                        continue
                    if plane == 0:
                        to = lax.rem(me_z + d, 4)
                        device, dst = at(to, me_x, c), final.at[piece, 0, me_z, :, me_c]
                    else:
                        to = lax.rem(me_x + d, 4)
                        device, dst = at(me_z, to, c), final.at[piece, 1, :, me_x, me_c]
                    pltpu.make_async_remote_copy(
                        src_ref=p1recv.at[piece, plane, :, to, c], dst_ref=dst,
                        send_sem=p2s_sem.at[piece], recv_sem=p2r_sem.at[piece],
                        device_id=device, device_id_type=MESH,
                    ).start()
        final[piece, 0, me_z, :, me_c] = p1recv[piece, 0, :, me_z, me_c]
        final[piece, 1, :, me_x, me_c] = p1recv[piece, 1, :, me_x, me_c]

    def seven_eighths(piece):
        return final.at[piece].reshape(512, 128).at[pl.ds(0, 448)]

    def z_stage(field):
        for pair in range(4):
            arrived = seven_eighths(field * 4 + pair)
            pltpu.make_async_copy(arrived, arrived, p2r_sem.at[field * 4 + pair]).wait()
        for ky in range(8):
            data = jnp.concatenate(
                [
                    final.at[field * 4 + pair, plane].reshape(256, 128)[
                        pl.ds(ky, 32, stride=8), :
                    ]
                    for pair in range(4)
                    for plane in range(2)
                ],
                axis=0,
            )
            high, low = split(data.T)
            out = dot(high, z_high[...]) + dot(low, z_high[...]) + dot(high, z_low[...])
            for part in range(2):
                modes_ref.at[field, part].reshape(1024, 128)[pl.ds(ky, 128, stride=8), :] = out[
                    :, 128 * part : 128 * part + 128
                ]

    for group in range(AHEAD):
        if group % 2 == 0:
            for copy in load_field(group // 2):
                copy.wait()
        x_stage(group // 2, group % 2)
        if group == 0:
            pl.semaphore_wait(barrier, len(peers))
        y_send(2 * group)
        y_send(2 * group + 1)

    @pl.loop(0, 8)
    def _(step):
        for part in range(2):
            piece = 2 * step + part
            y_stage(piece)
            first_send(piece)

            if part == 0:
                group = step + AHEAD

                @pl.when((group < 8) & (group % 2 == 0))
                def _():
                    for copy in load_field(group // 2):
                        copy.wait()

                @pl.when(group < 8)
                def _():
                    x_stage(group // 2, group % 2)
                    y_send(2 * group)
                    y_send(2 * group + 1)

            @pl.when(piece >= LAG)
            def _():
                second_send(piece - LAG)

        @pl.when((step == 4) | (step == 6))
        def _():
            z_stage((step - 4) // 2)

    for piece in range(16 - LAG, 16):
        second_send(piece)
    z_stage(2)
    z_stage(3)

    @pl.loop(0, 16)
    def _(piece):
        sent = ysend.at[piece, pl.ds(0, 3)]
        pltpu.make_async_copy(sent, sent, ys_sem.at[piece]).wait()
        sent = p1recv.at[piece, :, pl.ds(0, 3)]
        pltpu.make_async_copy(sent, sent, p1s_sem.at[piece]).wait()
        sent = seven_eighths(piece)
        pltpu.make_async_copy(sent, sent, p2s_sem.at[piece]).wait()


def exchange(species, table):
    dma = pltpu.SemaphoreType.DMA
    return pl.pallas_call(
        exchange_kernel,
        out_shape=jax.ShapeDtypeStruct((4, 2, 128, 8, 128), F32),
        in_specs=[
            pl.BlockSpec(memory_space=pl.ANY),
            pl.BlockSpec(memory_space=pltpu.VMEM),
        ],
        out_specs=pl.BlockSpec(memory_space=pltpu.VMEM),
        scratch_shapes=[
            pltpu.VMEM((4, 4, 64, 8, 128), F32),
            pltpu.VMEM((256, 512), BF16),
            pltpu.VMEM((256, 512), BF16),
            pltpu.VMEM((16, 4, 2, 64, 128), F32),
            pltpu.VMEM((16, 2, 4, 64, 128), F32),
            pltpu.VMEM((16, 2, 4, 4, 2, 8, 128), F32),
            pltpu.VMEM((16, 2, 4, 4, 2, 8, 128), F32),
            pltpu.VMEM((16, 2, 4, 4, 2, 8, 128), F32),
            dma((4, 4)),
            dma((16,)),
            dma((16,)),
            dma((16,)),
            dma((16, 2)),
            dma((16,)),
            dma((16,)),
        ],
        compiler_params=pltpu.CompilerParams(
            collective_id=0, has_side_effects=True, vmem_limit_bytes=48 * 2**20
        ),
        name="exchange",
    )(species, table)


def mix_kernel(modes_ref, coupling_ref, symbol_x_ref, symbol_y_ref, symbol_z_ref, out_ref):
    block = out_ref.shape[1]
    first = pl.program_id(0) * block
    first_x = lax.axis_index("py") * 128 + first
    first_y = lax.axis_index("pz") * 8
    row_y = lax.broadcasted_iota(jnp.int32, (8, 256), 0)
    symbol_yz = 1.0 + jnp.broadcast_to(symbol_z_ref[...], (8, 256))
    part_y = jnp.zeros((8, 256), F32)
    for k in range(8):
        part_y = jnp.where(row_y == k, symbol_y_ref[first_y + k], part_y)
    symbol_yz = symbol_yz + part_y

    for row in range(block):
        for part in range(2):
            lanes = slice(128 * part, 128 * part + 128)
            weight = 1.0 / (symbol_x_ref[first_x + row] + symbol_yz[:, lanes])
            old = [modes_ref[a, part, first + row] for a in range(4)]
            for a in range(4):
                mixed = coupling_ref[a, 0] * old[0]
                for b in range(1, 4):
                    mixed += coupling_ref[a, b] * old[b]
                out_ref[a, row, :, lanes] = mixed + weight * (old[a] - mixed)


def mix(modes, coupling, symbol_x, symbol_y, symbol_z):
    steps = 8
    block = 128 // steps
    smem = pl.BlockSpec(memory_space=pltpu.SMEM)
    return pl.pallas_call(
        mix_kernel,
        grid=(steps,),
        out_shape=jax.ShapeDtypeStruct((4, 128, 8, 256), F32),
        in_specs=[
            pl.BlockSpec(memory_space=pltpu.VMEM),
            smem,
            smem,
            smem,
            pl.BlockSpec(memory_space=pltpu.VMEM),
        ],
        out_specs=pl.BlockSpec((4, block, 8, 256), lambda i: (0, i, 0, 0)),
        compiler_params=pltpu.CompilerParams(vmem_limit_bytes=12 * 2**20),
        name="mix",
    )(modes, coupling, symbol_x, symbol_y, symbol_z.reshape(1, 256))


def shards(species, coupling, symbol_x, symbol_y, symbol_z):
    table_z = mode_table(256).reshape(32, 8, 256).transpose(1, 0, 2).reshape(256, 256)
    tables_yz = np.concatenate([halves(mode_table(256)), halves(table_z)], axis=1)
    table = np.concatenate([halves(mode_table(512)), tables_yz], axis=0)
    modes = exchange(species.transpose(0, 2, 3, 1), table)
    return mix(modes, coupling, symbol_x, symbol_y, symbol_z)


def solution(mesh):
    return jax.shard_map(
        shards,
        mesh=mesh,
        in_specs=(P(None, None, "py", "pz"), P(), P(), P(), P()),
        out_specs=P(None, "py", "pz", None),
        check_vma=False,
    )
```

```python
import functools

import jax
import jax.numpy as jnp
import numpy as np
from jax import lax
from jax.experimental import pallas as pl
from jax.experimental.pallas import tpu as pltpu
from jax.sharding import PartitionSpec as P

MESH = pl.DeviceIdType.MESH
F32 = jnp.float32
BF16 = jnp.bfloat16
AHEAD = 3
LAG = 2
MIX_STEPS = 8


def mode_table(count):
    rank = 2 * np.arange(count, dtype=np.int64) + 1
    angle = (rank[:, None] * rank[None, :] % (8 * count)) * (np.pi / (4 * count))
    return (np.cos(angle) * np.sqrt(2.0 / count)).astype(np.float32)


def halves(table):
    high = table.astype(BF16)
    low = (table - high.astype(np.float32)).astype(BF16)
    return np.concatenate([high, low], axis=0)


def split(values):
    high = values.astype(BF16)
    low = (values - high.astype(F32)).astype(BF16)
    return high, low


def dot(lhs, rhs):
    return jnp.dot(lhs, rhs, preferred_element_type=F32)


def exchange_kernel(
    species_ref, table_hbm, modes_ref,
    xin, table, lhs_high, lhs_low, ysend, yrecv, p1send, p1recv, final,
    in_sem, table_sem, ys_sem, yr_sem, p1s_sem, p1r_sem, p2s_sem, p2r_sem,
):
    me_y = lax.axis_index("py")
    me_pz = lax.axis_index("pz")
    me_z = me_pz // 8
    me_x = (me_pz // 2) % 4
    me_c = me_pz % 2

    def at(z, x, c):
        return (me_y, z * 8 + x * 2 + c)

    def load_field(field):
        return [
            pltpu.make_async_copy(
                species_ref.at[field, :, :, pl.ds(128 * tile, 128)],
                xin.at[field, tile],
                in_sem.at[field, tile],
            )
            for tile in range(4)
        ]

    y_high = table.at[pl.ds(1024, 256), pl.ds(0, 256)]
    y_low = table.at[pl.ds(1280, 256), pl.ds(0, 256)]
    z_high = table.at[pl.ds(1024, 256), pl.ds(256, 256)]
    z_low = table.at[pl.ds(1280, 256), pl.ds(256, 256)]

    tables = [
        pltpu.make_async_copy(table_hbm.at[rows], table.at[rows], table_sem.at[k])
        for k, rows in enumerate((pl.ds(0, 1024), pl.ds(1024, 512)))
    ]
    for copy in load_field(0):
        copy.start()
    tables[0].start()

    barrier = pltpu.get_barrier_semaphore()
    peers = [(lax.rem(me_y + d, 4), me_pz) for d in (1, 2, 3)]
    for d in (1, 2, 3):
        for c in (0, 1):
            peers.append(at(me_z, lax.rem(me_x + d, 4), c))
            peers.append(at(lax.rem(me_z + d, 4), me_x, c))
    peers.append(at(me_z, me_x, 1 - me_c))
    for peer in peers:
        pl.semaphore_signal(barrier, inc=1, device_id=peer, device_id_type=MESH)

    for field in (1, 2, 3):
        for copy in load_field(field):
            copy.start()
    tables[1].start()

    def x_stage(field, half):
        for plane in range(4):
            for tile in range(4):
                rows = xin.at[field, tile].reshape(512, 128)[
                    pl.ds(4 * half + plane, 64, stride=8), :
                ]
                high, low = split(rows)
                lhs_high[pl.ds(64 * plane, 64), pl.ds(128 * tile, 128)] = high
                lhs_low[pl.ds(64 * plane, 64), pl.ds(128 * tile, 128)] = low
        for side in range(2):
            columns = pl.ds(256 * side, 256)
            x_high = table[pl.ds(0, 512), columns]
            out = dot(lhs_high[...], x_high) + dot(lhs_low[...], x_high)
            out += dot(lhs_high[...], table[pl.ds(512, 512), columns])
            for plane in range(4):
                for part in range(2):
                    ysend[
                        field * 4 + half * 2 + plane // 2, side * 2 + part, plane % 2
                    ] = out[64 * plane : 64 * plane + 64, 128 * part : 128 * part + 128]

    def y_send(piece):
        for d in (1, 3, 2):
            to = lax.rem(me_y + d, 4)
            pltpu.make_async_remote_copy(
                src_ref=ysend.at[piece, to],
                dst_ref=yrecv.at[piece, :, me_y],
                send_sem=ys_sem.at[piece],
                recv_sem=yr_sem.at[piece],
                device_id=(to, me_pz),
                device_id_type=MESH,
            ).start()
        yrecv[piece, :, me_y] = ysend[piece, me_y]

    def y_stage(piece):
        all_y = yrecv.at[piece, :, pl.ds(0, 3)]
        pltpu.make_async_copy(all_y, all_y, yr_sem.at[piece]).wait()
        data = jnp.concatenate(
            [yrecv[piece, plane].reshape(256, 128) for plane in range(2)], axis=1
        )
        high, low = split(data)
        out = dot(y_high[...], high) + dot(y_low[...], high) + dot(y_high[...], low)
        for plane in range(2):
            p1send[piece, plane] = out[:, 128 * plane : 128 * plane + 128].reshape(
                4, 4, 2, 8, 128
            )

    def first_send(piece):
        for d in (1, 3, 2):
            for plane in range(2):
                if plane == 0:
                    to = lax.rem(me_x + d, 4)
                    src, device = p1send.at[piece, 0, :, to], at(me_z, to, me_c)
                    dst = p1recv.at[piece, 0, me_x]
                else:
                    to = lax.rem(me_z + d, 4)
                    src, device = p1send.at[piece, 1, to], at(to, me_x, me_c)
                    dst = p1recv.at[piece, 1, me_z]
                pltpu.make_async_remote_copy(
                    src_ref=src, dst_ref=dst,
                    send_sem=p1s_sem.at[piece], recv_sem=p1r_sem.at[piece, plane],
                    device_id=device, device_id_type=MESH,
                ).start()
        p1recv[piece, 0, me_x] = p1send[piece, 0, :, me_x]
        p1recv[piece, 1, me_z] = p1send[piece, 1, me_z]

    def second_send(piece):
        for plane in range(2):
            arrived = p1recv.at[piece, plane, pl.ds(0, 3)]
            pltpu.make_async_copy(arrived, arrived, p1r_sem.at[piece, plane]).wait()
            for d in (1, 3, 2, 0):
                for c in (me_c, 1 - me_c):
                    if d == 0 and c is me_c:
                        continue
                    if plane == 0:
                        to = lax.rem(me_z + d, 4)
                        device, dst = at(to, me_x, c), final.at[piece, 0, me_z, :, me_c]
                    else:
                        to = lax.rem(me_x + d, 4)
                        device, dst = at(me_z, to, c), final.at[piece, 1, :, me_x, me_c]
                    pltpu.make_async_remote_copy(
                        src_ref=p1recv.at[piece, plane, :, to, c], dst_ref=dst,
                        send_sem=p2s_sem.at[piece], recv_sem=p2r_sem.at[piece],
                        device_id=device, device_id_type=MESH,
                    ).start()
        final[piece, 0, me_z, :, me_c] = p1recv[piece, 0, :, me_z, me_c]
        final[piece, 1, :, me_x, me_c] = p1recv[piece, 1, :, me_x, me_c]

    def seven_eighths(piece):
        return final.at[piece].reshape(512, 128).at[pl.ds(0, 448)]

    def z_stage(field):
        for pair in range(4):
            arrived = seven_eighths(field * 4 + pair)
            pltpu.make_async_copy(arrived, arrived, p2r_sem.at[field * 4 + pair]).wait()
        for ky in range(8):
            data = jnp.concatenate(
                [
                    final.at[field * 4 + pair, plane].reshape(256, 128)[
                        pl.ds(ky, 32, stride=8), :
                    ]
                    for pair in range(4)
                    for plane in range(2)
                ],
                axis=0,
            )
            high, low = split(data.T)
            out = dot(high, z_high[...]) + dot(low, z_high[...]) + dot(high, z_low[...])
            for part in range(2):
                modes_ref.at[field, part].reshape(1024, 128)[pl.ds(ky, 128, stride=8), :] = out[
                    :, 128 * part : 128 * part + 128
                ]

    tables[0].wait()
    for group in range(AHEAD):
        if group % 2 == 0:
            for copy in load_field(group // 2):
                copy.wait()
        x_stage(group // 2, group % 2)
        if group == 0:
            pl.semaphore_wait(barrier, len(peers))
        y_send(2 * group)
        y_send(2 * group + 1)

    tables[1].wait()

    @pl.loop(0, 8)
    def _(step):
        for part in range(2):
            piece = 2 * step + part
            y_stage(piece)
            first_send(piece)

            if part == 0:
                group = step + AHEAD

                @pl.when((group < 8) & (group % 2 == 0))
                def _():
                    for copy in load_field(group // 2):
                        copy.wait()

                @pl.when(group < 8)
                def _():
                    x_stage(group // 2, group % 2)
                    y_send(2 * group)
                    y_send(2 * group + 1)

            @pl.when(piece >= LAG)
            def _():
                second_send(piece - LAG)

        @pl.when((step == 4) | (step == 6))
        def _():
            z_stage((step - 4) // 2)

    for piece in range(16 - LAG, 16):
        second_send(piece)
    z_stage(2)
    z_stage(3)

    @pl.loop(0, 16)
    def _(piece):
        sent = ysend.at[piece, pl.ds(0, 3)]
        pltpu.make_async_copy(sent, sent, ys_sem.at[piece]).wait()
        sent = p1recv.at[piece, :, pl.ds(0, 3)]
        pltpu.make_async_copy(sent, sent, p1s_sem.at[piece]).wait()
        sent = seven_eighths(piece)
        pltpu.make_async_copy(sent, sent, p2s_sem.at[piece]).wait()


def exchange(species, table):
    dma = pltpu.SemaphoreType.DMA
    return pl.pallas_call(
        exchange_kernel,
        out_shape=pltpu.VMEM((4, 2, 128, 8, 128), F32),
        in_specs=[
            pl.BlockSpec(memory_space=pl.ANY),
            pl.BlockSpec(memory_space=pl.ANY),
        ],
        out_specs=pl.BlockSpec(memory_space=pltpu.VMEM),
        scratch_shapes=[
            pltpu.VMEM((4, 4, 64, 8, 128), F32),
            pltpu.VMEM((1536, 512), BF16),
            pltpu.VMEM((256, 512), BF16),
            pltpu.VMEM((256, 512), BF16),
            pltpu.VMEM((16, 4, 2, 64, 128), F32),
            pltpu.VMEM((16, 2, 4, 64, 128), F32),
            pltpu.VMEM((16, 2, 4, 4, 2, 8, 128), F32),
            pltpu.VMEM((16, 2, 4, 4, 2, 8, 128), F32),
            pltpu.VMEM((16, 2, 4, 4, 2, 8, 128), F32),
            dma((4, 4)),
            dma((2,)),
            dma((16,)),
            dma((16,)),
            dma((16,)),
            dma((16, 2)),
            dma((16,)),
            dma((16,)),
        ],
        compiler_params=pltpu.CompilerParams(
            collective_id=0, has_side_effects=True, vmem_limit_bytes=54 * 2**20
        ),
        name="exchange",
    )(species, table)


def mix_kernel(
    modes_ref, coupling_ref, symbol_x_ref, symbol_y_ref, symbol_z_ref, out_ref, mixed, out_sem
):
    block = 128 // MIX_STEPS
    first_x = lax.axis_index("py") * 128
    first_y = lax.axis_index("pz") * 8
    row_y = lax.broadcasted_iota(jnp.int32, (8, 256), 0)
    symbol_yz = 1.0 + jnp.broadcast_to(symbol_z_ref[...], (8, 256))
    part_y = jnp.zeros((8, 256), F32)
    for k in range(8):
        part_y = jnp.where(row_y == k, symbol_y_ref[first_y + k], part_y)
    symbol_yz = symbol_yz + part_y

    def store(step):
        rows = pl.ds(block * step, block)
        return pltpu.make_async_copy(mixed.at[:, rows], out_ref.at[:, rows], out_sem.at[step])

    @pl.loop(0, MIX_STEPS)
    def _(step):
        for k in range(block):
            row = block * step + k
            for part in range(2):
                lanes = slice(128 * part, 128 * part + 128)
                weight = 1.0 / (symbol_x_ref[first_x + row] + symbol_yz[:, lanes])
                old = [modes_ref[a, part, row] for a in range(4)]
                for a in range(4):
                    total = coupling_ref[a, 0] * old[0]
                    for b in range(1, 4):
                        total += coupling_ref[a, b] * old[b]
                    mixed[a, row, :, lanes] = total + weight * (old[a] - total)
        store(step).start()

    for step in range(MIX_STEPS):
        store(step).wait()


def mix(modes, coupling, symbol_x, symbol_y, symbol_z):
    smem = pl.BlockSpec(memory_space=pltpu.SMEM)
    return pl.pallas_call(
        mix_kernel,
        out_shape=jax.ShapeDtypeStruct((4, 128, 8, 256), F32),
        in_specs=[
            pl.BlockSpec(memory_space=pltpu.VMEM),
            smem,
            smem,
            smem,
            pl.BlockSpec(memory_space=pltpu.VMEM),
        ],
        out_specs=pl.BlockSpec(memory_space=pl.ANY),
        scratch_shapes=[
            pltpu.VMEM((4, 128, 8, 256), F32),
            pltpu.SemaphoreType.DMA((MIX_STEPS,)),
        ],
        compiler_params=pltpu.CompilerParams(vmem_limit_bytes=12 * 2**20),
        name="mix",
    )(modes, coupling, symbol_x, symbol_y, symbol_z.reshape(1, 256))


def shards(species, coupling, symbol_x, symbol_y, symbol_z):
    table_z = mode_table(256).reshape(32, 8, 256).transpose(1, 0, 2).reshape(256, 256)
    tables_yz = np.concatenate([halves(mode_table(256)), halves(table_z)], axis=1)
    table = np.concatenate([halves(mode_table(512)), tables_yz], axis=0)
    modes = exchange(species.transpose(0, 2, 3, 1), table)
    return mix(modes, coupling, symbol_x, symbol_y, symbol_z)


def solution(mesh):
    return jax.shard_map(
        shards,
        mesh=mesh,
        in_specs=(P(None, None, "py", "pz"), P(), P(), P(), P()),
        out_specs=P(None, "py", "pz", None),
        check_vma=False,
    )
```

```python
import functools

import jax
import jax.numpy as jnp
import numpy as np
from jax import lax
from jax.experimental import pallas as pl
from jax.experimental.pallas import tpu as pltpu
from jax.sharding import PartitionSpec as P

MESH = pl.DeviceIdType.MESH
F32 = jnp.float32
BF16 = jnp.bfloat16
AHEAD = 3
LAG = 2
MIX_STEPS = 8


def mode_table(count):
    rank = 2 * np.arange(count, dtype=np.int64) + 1
    angle = (rank[:, None] * rank[None, :] % (8 * count)) * (np.pi / (4 * count))
    return (np.cos(angle) * np.sqrt(2.0 / count)).astype(np.float32)


def halves(table):
    high = table.astype(BF16)
    low = (table - high.astype(np.float32)).astype(BF16)
    return np.concatenate([high, low], axis=0)


def split(values):
    high = values.astype(BF16)
    low = (values - high.astype(F32)).astype(BF16)
    return high, low


def dot(lhs, rhs):
    return jnp.dot(lhs, rhs, preferred_element_type=F32)


def exchange_kernel(
    species_ref, table_hbm, coupling_hbm, symbol_x_hbm, symbol_y_hbm, symbol_z_hbm,
    modes_ref, weight_ref, coupling_ref,
    coupling, symbol_x, symbol_y, symbol_z, xin, table, lhs_high, lhs_low, ysend, yrecv, p1send, p1recv, final,
    in_sem, table_sem, small_sem, ys_sem, yr_sem, p1s_sem, p1r_sem, p2s_sem, p2r_sem,
):
    me_y = lax.axis_index("py")
    me_pz = lax.axis_index("pz")
    me_z = me_pz // 8
    me_x = (me_pz // 2) % 4
    me_c = me_pz % 2

    def at(z, x, c):
        return (me_y, z * 8 + x * 2 + c)

    def load_field(field):
        return [
            pltpu.make_async_copy(
                species_ref.at[field, :, :, pl.ds(128 * tile, 128)],
                xin.at[field, tile],
                in_sem.at[field, tile],
            )
            for tile in range(4)
        ]

    y_high = table.at[pl.ds(1024, 256), pl.ds(0, 256)]
    y_low = table.at[pl.ds(1280, 256), pl.ds(0, 256)]
    z_high = table.at[pl.ds(1024, 256), pl.ds(256, 256)]
    z_low = table.at[pl.ds(1280, 256), pl.ds(256, 256)]

    tables = [
        pltpu.make_async_copy(table_hbm.at[rows], table.at[rows], table_sem.at[k])
        for k, rows in enumerate((pl.ds(0, 1024), pl.ds(1024, 512)))
    ]
    for copy in load_field(0):
        copy.start()
    tables[0].start()

    barrier = pltpu.get_barrier_semaphore()
    peers = [(lax.rem(me_y + d, 4), me_pz) for d in (1, 2, 3)]
    for d in (1, 2, 3):
        for c in (0, 1):
            peers.append(at(me_z, lax.rem(me_x + d, 4), c))
            peers.append(at(lax.rem(me_z + d, 4), me_x, c))
    peers.append(at(me_z, me_x, 1 - me_c))
    for peer in peers:
        pl.semaphore_signal(barrier, inc=1, device_id=peer, device_id_type=MESH)

    for field in (1, 2, 3):
        for copy in load_field(field):
            copy.start()
    tables[1].start()
    smalls = [
        pltpu.make_async_copy(coupling_hbm, coupling, small_sem.at[0]),
        pltpu.make_async_copy(symbol_x_hbm, symbol_x, small_sem.at[1]),
        pltpu.make_async_copy(symbol_y_hbm, symbol_y, small_sem.at[2]),
        pltpu.make_async_copy(symbol_z_hbm, symbol_z, small_sem.at[3]),
    ]
    for copy in smalls:
        copy.start()

    def weights(step):
        row_y = lax.broadcasted_iota(jnp.int32, (8, 128), 0)
        for part in range(2):
            lanes = pl.ds(128 * part, 128)
            symbol_yz = 1.0 + jnp.broadcast_to(symbol_z[:, lanes], (8, 128))
            part_y = jnp.zeros((8, 128), F32)
            for k in range(8):
                part_y = jnp.where(row_y == k, symbol_y[me_pz * 8 + k], part_y)
            symbol_yz = symbol_yz + part_y
            for k in range(16):
                row = 16 * step + k
                weight_ref[part, row] = 1.0 / (symbol_x[me_y * 128 + row] + symbol_yz)

    def x_stage(field, half):
        for plane in range(4):
            for tile in range(4):
                rows = xin.at[field, tile].reshape(512, 128)[
                    pl.ds(4 * half + plane, 64, stride=8), :
                ]
                high, low = split(rows)
                lhs_high[pl.ds(64 * plane, 64), pl.ds(128 * tile, 128)] = high
                lhs_low[pl.ds(64 * plane, 64), pl.ds(128 * tile, 128)] = low
        for side in range(2):
            columns = pl.ds(256 * side, 256)
            x_high = table[pl.ds(0, 512), columns]
            out = dot(lhs_high[...], x_high) + dot(lhs_low[...], x_high)
            out += dot(lhs_high[...], table[pl.ds(512, 512), columns])
            for plane in range(4):
                for part in range(2):
                    ysend[
                        field * 4 + half * 2 + plane // 2, side * 2 + part, plane % 2
                    ] = out[64 * plane : 64 * plane + 64, 128 * part : 128 * part + 128]

    def y_send(piece):
        for d in (2, 1, 3):
            to = lax.rem(me_y + d, 4)
            pltpu.make_async_remote_copy(
                src_ref=ysend.at[piece, to],
                dst_ref=yrecv.at[piece, :, me_y],
                send_sem=ys_sem.at[piece],
                recv_sem=yr_sem.at[piece],
                device_id=(to, me_pz),
                device_id_type=MESH,
            ).start()
        yrecv[piece, :, me_y] = ysend[piece, me_y]

    def y_stage(piece):
        all_y = yrecv.at[piece, :, pl.ds(0, 3)]
        pltpu.make_async_copy(all_y, all_y, yr_sem.at[piece]).wait()
        data = jnp.concatenate(
            [yrecv[piece, plane].reshape(256, 128) for plane in range(2)], axis=1
        )
        high, low = split(data)
        out = dot(y_high[...], high) + dot(y_low[...], high) + dot(y_high[...], low)
        for plane in range(2):
            p1send[piece, plane] = out[:, 128 * plane : 128 * plane + 128].reshape(
                4, 4, 2, 8, 128
            )

    def first_send(piece):
        for d in (2, 1, 3):
            for plane in range(2):
                if plane == 0:
                    to = lax.rem(me_x + d, 4)
                    src, device = p1send.at[piece, 0, :, to], at(me_z, to, me_c)
                    dst = p1recv.at[piece, 0, me_x]
                else:
                    to = lax.rem(me_z + d, 4)
                    src, device = p1send.at[piece, 1, to], at(to, me_x, me_c)
                    dst = p1recv.at[piece, 1, me_z]
                pltpu.make_async_remote_copy(
                    src_ref=src, dst_ref=dst,
                    send_sem=p1s_sem.at[piece], recv_sem=p1r_sem.at[piece, plane],
                    device_id=device, device_id_type=MESH,
                ).start()
        p1recv[piece, 0, me_x] = p1send[piece, 0, :, me_x]
        p1recv[piece, 1, me_z] = p1send[piece, 1, me_z]

    def second_send(piece):
        for plane in range(2):
            arrived = p1recv.at[piece, plane, pl.ds(0, 3)]
            pltpu.make_async_copy(arrived, arrived, p1r_sem.at[piece, plane]).wait()
            for d in (2, 1, 3, 0):
                for c in (me_c, 1 - me_c):
                    if d == 0 and c is me_c:
                        continue
                    if plane == 0:
                        to = lax.rem(me_z + d, 4)
                        device, dst = at(to, me_x, c), final.at[piece, 0, me_z, :, me_c]
                    else:
                        to = lax.rem(me_x + d, 4)
                        device, dst = at(me_z, to, c), final.at[piece, 1, :, me_x, me_c]
                    pltpu.make_async_remote_copy(
                        src_ref=p1recv.at[piece, plane, :, to, c], dst_ref=dst,
                        send_sem=p2s_sem.at[piece], recv_sem=p2r_sem.at[piece],
                        device_id=device, device_id_type=MESH,
                    ).start()
        final[piece, 0, me_z, :, me_c] = p1recv[piece, 0, :, me_z, me_c]
        final[piece, 1, :, me_x, me_c] = p1recv[piece, 1, :, me_x, me_c]

    def seven_eighths(piece):
        return final.at[piece].reshape(512, 128).at[pl.ds(0, 448)]

    def z_stage(field):
        for pair in range(4):
            arrived = seven_eighths(field * 4 + pair)
            pltpu.make_async_copy(arrived, arrived, p2r_sem.at[field * 4 + pair]).wait()
        for ky in range(8):
            data = jnp.concatenate(
                [
                    final.at[field * 4 + pair, plane].reshape(256, 128)[
                        pl.ds(ky, 32, stride=8), :
                    ]
                    for pair in range(4)
                    for plane in range(2)
                ],
                axis=0,
            )
            high, low = split(data.T)
            out = dot(high, z_high[...]) + dot(low, z_high[...]) + dot(high, z_low[...])
            for part in range(2):
                modes_ref.at[field, part].reshape(1024, 128)[pl.ds(ky, 128, stride=8), :] = out[
                    :, 128 * part : 128 * part + 128
                ]

    tables[0].wait()
    for group in range(AHEAD):
        if group % 2 == 0:
            for copy in load_field(group // 2):
                copy.wait()
        x_stage(group // 2, group % 2)
        if group == 0:
            pl.semaphore_wait(barrier, len(peers))
        y_send(2 * group)
        y_send(2 * group + 1)

    tables[1].wait()
    for copy in smalls:
        copy.wait()
    for a in range(4):
        for b in range(4):
            coupling_ref[4 * a + b] = jnp.full((8, 128), coupling[a, b], F32)

    @pl.loop(0, 8)
    def _(step):
        for part in range(2):
            piece = 2 * step + part
            y_stage(piece)
            first_send(piece)

            if part == 0:
                group = step + AHEAD

                @pl.when((group < 8) & (group % 2 == 0))
                def _():
                    for copy in load_field(group // 2):
                        copy.wait()

                @pl.when(group < 8)
                def _():
                    x_stage(group // 2, group % 2)
                    y_send(2 * group)
                    y_send(2 * group + 1)

            @pl.when(piece >= LAG)
            def _():
                second_send(piece - LAG)

        weights(step)

        @pl.when((step == 4) | (step == 6))
        def _():
            z_stage((step - 4) // 2)

    for piece in range(16 - LAG, 16):
        second_send(piece)
    z_stage(2)
    z_stage(3)

    @pl.loop(0, 16)
    def _(piece):
        sent = ysend.at[piece, pl.ds(0, 3)]
        pltpu.make_async_copy(sent, sent, ys_sem.at[piece]).wait()
        sent = p1recv.at[piece, :, pl.ds(0, 3)]
        pltpu.make_async_copy(sent, sent, p1s_sem.at[piece]).wait()
        sent = seven_eighths(piece)
        pltpu.make_async_copy(sent, sent, p2s_sem.at[piece]).wait()


def exchange(species, table, coupling, symbol_x, symbol_y, symbol_z):
    dma = pltpu.SemaphoreType.DMA
    return pl.pallas_call(
        exchange_kernel,
        out_shape=(
            pltpu.VMEM((4, 2, 128, 8, 128), F32),
            pltpu.VMEM((2, 128, 8, 128), F32),
            pltpu.VMEM((16, 8, 128), F32),
        ),
        in_specs=[pl.BlockSpec(memory_space=pl.ANY)] * 6,
        out_specs=[pl.BlockSpec(memory_space=pltpu.VMEM)] * 3,
        scratch_shapes=[
            pltpu.SMEM((4, 4), F32),
            pltpu.SMEM((512,), F32),
            pltpu.SMEM((256,), F32),
            pltpu.VMEM((1, 256), F32),
            pltpu.VMEM((4, 4, 64, 8, 128), F32),
            pltpu.VMEM((1536, 512), BF16),
            pltpu.VMEM((256, 512), BF16),
            pltpu.VMEM((256, 512), BF16),
            pltpu.VMEM((16, 4, 2, 64, 128), F32),
            pltpu.VMEM((16, 2, 4, 64, 128), F32),
            pltpu.VMEM((16, 2, 4, 4, 2, 8, 128), F32),
            pltpu.VMEM((16, 2, 4, 4, 2, 8, 128), F32),
            pltpu.VMEM((16, 2, 4, 4, 2, 8, 128), F32),
            dma((4, 4)),
            dma((2,)),
            dma((4,)),
            dma((16,)),
            dma((16,)),
            dma((16,)),
            dma((16, 2)),
            dma((16,)),
            dma((16,)),
        ],
        compiler_params=pltpu.CompilerParams(
            collective_id=0, has_side_effects=True, vmem_limit_bytes=54 * 2**20
        ),
        name="exchange",
    )(species, table, coupling, symbol_x, symbol_y, symbol_z.reshape(1, 256))


def mix_kernel(modes_ref, weight_ref, coupling_ref, out_ref, mixed, out_sem):
    block = 128 // MIX_STEPS

    def store(step):
        rows = pl.ds(block * step, block)
        return pltpu.make_async_copy(mixed.at[:, rows], out_ref.at[:, rows], out_sem.at[step])

    @pl.loop(0, MIX_STEPS)
    def _(step):
        for k in range(block):
            row = block * step + k
            for part in range(2):
                lanes = slice(128 * part, 128 * part + 128)
                weight = weight_ref[part, row]
                old = [modes_ref[a, part, row] for a in range(4)]
                for a in range(4):
                    total = coupling_ref[4 * a] * old[0]
                    for b in range(1, 4):
                        total += coupling_ref[4 * a + b] * old[b]
                    mixed[a, row, :, lanes] = total + weight * (old[a] - total)
        store(step).start()

    for step in range(MIX_STEPS):
        store(step).wait()


def mix(modes, weight, coupling):
    return pl.pallas_call(
        mix_kernel,
        out_shape=jax.ShapeDtypeStruct((4, 128, 8, 256), F32),
        in_specs=[pl.BlockSpec(memory_space=pltpu.VMEM)] * 3,
        out_specs=pl.BlockSpec(memory_space=pl.ANY),
        scratch_shapes=[
            pltpu.VMEM((4, 128, 8, 256), F32),
            pltpu.SemaphoreType.DMA((MIX_STEPS,)),
        ],
        compiler_params=pltpu.CompilerParams(vmem_limit_bytes=12 * 2**20),
        name="mix",
    )(modes, weight, coupling)


def shards(species, coupling, symbol_x, symbol_y, symbol_z):
    table_z = mode_table(256).reshape(32, 8, 256).transpose(1, 0, 2).reshape(256, 256)
    tables_yz = np.concatenate([halves(mode_table(256)), halves(table_z)], axis=1)
    table = np.concatenate([halves(mode_table(512)), tables_yz], axis=0)
    modes, weight, splats = exchange(
        species.transpose(0, 2, 3, 1), table, coupling, symbol_x, symbol_y, symbol_z
    )
    return mix(modes, weight, splats)


def solution(mesh):
    return jax.shard_map(
        shards,
        mesh=mesh,
        in_specs=(P(None, None, "py", "pz"), P(), P(), P(), P()),
        out_specs=P(None, "py", "pz", None),
        check_vma=False,
    )
```
